32 devices in a mesh: seq: 4 (over z), exp: 8 (over y, x, core).
Axes of the slice: x: 2, y: 2, z: 4, core: 2. Of those that a mesh axis runs over, the one named last changes fastest.
Arguments:
- residual_in: bfloat16 [1024, 8, 1152], P('seq', 'exp'), may hold values from -6 to 6
- query_proj: bfloat16 [1024, 8, 1152], P('seq', 'exp'), may hold values from -6 to 6
- key_proj: bfloat16 [1024, 8, 1152], P('seq', 'exp'), may hold values from -6 to 6
- value_proj: bfloat16 [1024, 8, 1152], P('seq', 'exp'), may hold values from -6 to 6
- out_weight: bfloat16 [1152, 1152], replicated, may hold values from -0.1875 to 0.1875
- router_weight: bfloat16 [1152, 4], replicated, may hold values from -0.1875 to 0.1875
- first_weight: bfloat16 [8, 1152, 2304], P('exp', None, 'seq'), may hold values from -0.1875 to 0.1875
- second_weight: bfloat16 [8, 2304, 1152], P('exp', 'seq'), may hold values from -0.09375 to 0.09375
- class_table: bfloat16 [1024, 4, 1152], P('seq'), may hold values from -3 to 3
- time_weight: bfloat16 [256, 4, 1152], P('seq'), may hold values from -0.375 to 0.375
- class_labels: int32 [8], P('exp'), may hold values from 0 to 1023
- timesteps: int32 [8], P('exp'), may hold values from 0 to 999
- expert_ids: int32 [4, 8, 256, 1, 2], P('seq', 'exp'), may hold values from 0 to 3, all different within a row; in each aligned block of 256 rows (0 to 255, 256 to 511, ..., all dimensions but the last counted through in order) at most 160 rows name the same one
Outputs:
- block_out: bfloat16 [1024, 8, 1152], P('seq', 'exp')
The draws below stay inside these ranges and needn't reach their ends.
Inputs may be any that keep to these rules, and one draw needn't show every extreme that they name: `expert_ids`: each row names 2 different experts; among the rows of one device no expert is named by more than 160 rows.
All inputs are finite; a program needn't handle non-finite values.
Results may differ from the reference program's by a relative error of at most 0.013.
Values may be sent and summed in bfloat16 or wider, within the bound.
No kernel may reach another device: no remote copies, remote signals or barrier semaphores. Data moves between devices by JAX's collectives and lax.ppermute only.
A program may use at most 128 MiB of HBM per device.

```python
import math
import jax
import jax.numpy as jnp
import numpy as np
from jax import lax

D = 1152
HEAD = 72
HEADS_WIN = 16
FFW = 4608
TOP = 2
FREQ = 256
CLASSES = 1024
LEN = 1024
IMG_DEV = 1
SEQ_DEV = 256
TOK_DEV = 256
IMAGES = 8
EXPERTS = 4
HW = 1152
CAP = 160
N_SEQ = 4
N_EXP = 8


def draw_key_proj(key, part):
    values = jnp.clip(jax.random.normal(jax.random.fold_in(key, 11), (LEN, IMAGES, HW), jnp.float32), -6.0, 6.0)
    return values.astype(jnp.bfloat16)


def draw_query_proj(key, part):
    values = jnp.clip(jax.random.normal(jax.random.fold_in(key, 21), (LEN, IMAGES, HW), jnp.float32), -6.0, 6.0)
    return values.astype(jnp.bfloat16)


def plant(values, key, low, high):
    shape = values.shape
    place = [jax.random.randint(jax.random.fold_in(key, axis), (), 0, shape[axis]) for axis in range(len(shape))]
    values = values.at[tuple(place)].set(low)
    longest = shape.index(max(shape))
    place[longest] = (place[longest] + 1) % shape[longest]
    return values.at[tuple(place)].set(high)


def steps_of(own_key, shape, shards, least, largest):
    def one(position, blocks):
        draws = jax.random.uniform(jax.random.fold_in(jax.random.fold_in(own_key, 6), position), (blocks,), jnp.float32, least / len(shards), largest / len(shards))
        return jnp.repeat(jnp.exp(draws), shape[position] // blocks).reshape((-1,) + (1,) * (len(shape) - position - 1))

    factor_of = one(*shards[0])
    for cut in shards[1:]:
        factor_of = factor_of * one(*cut)
    return factor_of


def routed_block(own_key, own, number, rows, number_of, top, limit, slope):
    order = jax.random.permutation(own_key, number_of)
    heavy_load, usual = load_shares(number_of, rows * top, limit, slope, True), load_shares(number_of, rows * top, limit, slope, False)
    places = jnp.arange(number_of)

    def named(lengths, turn):
        used = int((lengths > 0).sum())
        fixed = max(1, used // 4)
        passed = fixed + (places - fixed + turn * (used - fixed)) % max(1, number_of - fixed)
        return jnp.zeros((number_of,), jnp.int32).at[order[jnp.where(places < fixed, places, passed)]].set(jnp.asarray(lengths, jnp.int32))

    lengths = jnp.where(number % 4 == 0, named(heavy_load, number // 4), named(usual, number - number // 4 - 1))
    mixed = jax.random.permutation(jax.random.fold_in(own, 3), number_of)
    source_of, sink = mixed[0:number_of // 2 * 2:2], mixed[1:number_of // 2 * 2:2]
    margin = jnp.minimum(lengths[source_of] - 1, limit - lengths[sink]) // 2
    margin = jnp.where((source_of == order[0]) | (sink == order[0]) | (lengths[sink] == 0), 0, jnp.maximum(margin, 0))
    passed = jax.random.randint(jax.random.fold_in(own, 4), (number_of // 2,), 0, 1 << 20) % (margin + 1)
    lengths = lengths.at[source_of].add(-passed).at[sink].add(passed)
    items = jnp.searchsorted(jnp.cumsum(lengths), jnp.arange(rows * top), side="right").astype(jnp.int32)
    grid = items.reshape(top, rows).T
    grid = grid[jax.random.permutation(jax.random.fold_in(own, 1), rows)]
    turn = jax.random.randint(jax.random.fold_in(own, 2), (rows, 1), 0, top)
    return jnp.take_along_axis(grid, (jnp.arange(top)[None, :] + turn) % top, axis=1)


def load_shares(count, total, bound, skew, full):
    loads = [(1 << 20) // math.isqrt(rank ** skew) + 1 for rank in range(1, count + 1)]
    largest = bound if full else min(bound, max(-(-total // count), total * loads[0] // sum(loads)))
    least = 1 if total - largest >= count - 1 else 0
    given, surplus = [largest] + [least] * (count - 1), total - largest - least * (count - 1)
    while surplus > 0:
        movable = [i for i in range(1, count) if given[i] < largest] or [i for i in range(1, count) if given[i] < bound]
        mass, remaining = sum([loads[i] for i in movable]), surplus
        for i in movable:
            extra = min(bound - given[i], max(1, remaining * loads[i] // mass), surplus)
            given[i] = given[i] + extra
            surplus = surplus - extra
    return np.array(given)


def scatter_about(rng, extent, deviation, most, pieces=(), kind=jnp.bfloat16):
    loudness = steps_of(rng, extent, pieces, -0.22, 0.18) if pieces else 1.0
    values = jax.random.normal(rng, extent, jnp.float32) * deviation * loudness
    return jnp.minimum(jnp.maximum(values, -most), most).astype(kind)


def setup_inputs(seed: int = 0) -> dict:
    key_of = jax.random.split(jax.random.key(seed), 14)
    residual_in = scatter_about(key_of[0], (LEN, IMAGES, D), 1.0, 6.0, ((0, 4), (1, 8)))
    query_proj = draw_query_proj(jax.random.fold_in(key_of[13], 71), 0)
    key_proj = draw_key_proj(jax.random.fold_in(key_of[13], 71), 0)
    value_proj = scatter_about(key_of[3], (LEN, IMAGES, HW), 1.0, 6.0, ((0, 4), (1, 8)))
    out_weight = scatter_about(key_of[4], (HW, D), HW ** -0.5, 0.1875)
    router_weight = scatter_about(key_of[5], (D, EXPERTS), D ** -0.5, 0.1875)
    first_weight = scatter_about(key_of[6], (N_EXP, D, FFW // 2), D ** -0.5, 0.1875, ((0, 8), (2, 4)))
    second_weight = scatter_about(key_of[7], (N_EXP, FFW // 2, D), FFW ** -0.5, 0.09375, ((0, 8), (1, 4)))
    class_table = scatter_about(key_of[8], (CLASSES, 4, D), 0.5, 3.0, ((0, 4),))
    time_weight = scatter_about(key_of[9], (FREQ, 4, D), FREQ ** -0.5, 0.375, ((0, 4),))
    class_labels = plant(jax.random.randint(key_of[10], (IMAGES,), 0, CLASSES), jax.random.fold_in(key_of[10], 1), 0, CLASSES - 1).astype(jnp.int32)
    timesteps = plant(jax.random.randint(key_of[11], (IMAGES,), 0, 1000), jax.random.fold_in(key_of[11], 1), 0, 999).astype(jnp.int32)
    expert_ids_keys = jax.random.split(jax.random.fold_in(key_of[12], 1), N_SEQ * N_EXP * SEQ_DEV * IMG_DEV // TOK_DEV)
    expert_ids_turns = jax.random.permutation(jax.random.fold_in(key_of[12], 3), N_SEQ * N_EXP * SEQ_DEV * IMG_DEV // TOK_DEV)
    expert_ids = jax.vmap(lambda own, number: routed_block(jax.random.fold_in(key_of[12], 2), own, number, TOK_DEV, EXPERTS, TOP, CAP, 2))(expert_ids_keys, expert_ids_turns).reshape((N_SEQ, N_EXP, SEQ_DEV, IMG_DEV, TOP))
    return {"residual_in": residual_in, "query_proj": query_proj, "key_proj": key_proj, "value_proj": value_proj, "out_weight": out_weight, "router_weight": router_weight, "first_weight": first_weight, "second_weight": second_weight, "class_table": class_table, "time_weight": time_weight, "class_labels": class_labels, "timesteps": timesteps, "expert_ids": expert_ids}


def time_embed(timesteps):
    half_width = FREQ // 2
    frequencies = jnp.exp(-math.log(10000.0) * jnp.arange(half_width, dtype=jnp.float32) / half_width)
    angles = timesteps.astype(jnp.float32)[:, None] * frequencies[None, :]
    return jnp.concatenate([jnp.cos(angles), jnp.sin(angles)], axis=1)

def attend_image(operands):
    query_heads, key_heads, value_heads = operands
    inv_root = 1.0 / math.sqrt(HEAD)
    scores = jnp.einsum('qhe,khe->hqk', query_heads.astype(jnp.float32), key_heads.astype(jnp.float32)) * inv_root
    row_max = lax.optimization_barrier(jnp.max(scores, axis=-1, keepdims=True))
    exp_scores = jnp.exp(scores - row_max)
    row_total = lax.optimization_barrier(jnp.sum(exp_scores, axis=-1, keepdims=True))
    rounded_w = exp_scores.astype(jnp.bfloat16)
    mixed_out = jnp.einsum('hqk,khe->qhe', rounded_w.astype(jnp.float32), value_heads.astype(jnp.float32))
    return (mixed_out / jnp.transpose(row_total, (1, 0, 2))).astype(jnp.bfloat16)

def half_apply(block_rows, weight_one, weight_two):
    pre_act = jnp.dot(block_rows.astype(jnp.float32), weight_one.astype(jnp.float32), preferred_element_type=jnp.float32)
    inner_act = jax.nn.gelu(pre_act, approximate=True).astype(jnp.bfloat16)
    return jnp.dot(inner_act.astype(jnp.float32), weight_two.astype(jnp.float32), preferred_element_type=jnp.float32).astype(jnp.bfloat16)

def expert_apply(operands):
    block_rows, weight_one, weight_two = operands
    lower = half_apply(block_rows, weight_one[0], weight_two[0]).astype(jnp.float32)
    upper = half_apply(block_rows, weight_one[1], weight_two[1]).astype(jnp.float32)
    return (lower + upper).astype(jnp.bfloat16)

def to_blocks(array):
    tail = array.shape[2:]
    shaped = array.reshape((N_SEQ, LEN // N_SEQ, N_EXP, IMAGES // N_EXP) + tail)
    shaped = jnp.swapaxes(shaped, 1, 2)
    return shaped.reshape((N_SEQ * N_EXP, LEN // N_SEQ * (IMAGES // N_EXP)) + tail)

def from_blocks(array):
    tail = array.shape[2:]
    shaped = array.reshape((N_SEQ, N_EXP, LEN // N_SEQ, IMAGES // N_EXP) + tail)
    shaped = jnp.swapaxes(shaped, 1, 2)
    return shaped.reshape((LEN, IMAGES) + tail)

def reference(residual_in, query_proj, key_proj, value_proj, out_weight, router_weight, first_weight, second_weight, class_table, time_weight, class_labels, timesteps, expert_ids):
    table_rows = jnp.take(class_table, class_labels, axis=0).astype(jnp.float32)
    embedded = time_embed(timesteps)
    time_part = jnp.dot(embedded, time_weight.astype(jnp.float32).reshape(FREQ, 4 * D), precision=lax.Precision.HIGHEST)
    conditions = table_rows + time_part.reshape(IMAGES, 4, D)
    query_img = query_proj.reshape(LEN, IMAGES, HEADS_WIN, HEAD).transpose(1, 0, 2, 3)
    key_img = key_proj.reshape(LEN, IMAGES, HEADS_WIN, HEAD).transpose(1, 0, 2, 3)
    value_img = value_proj.reshape(LEN, IMAGES, HEADS_WIN, HEAD).transpose(1, 0, 2, 3)
    attended = lax.map(attend_image, (query_img, key_img, value_img))
    attended = attended.transpose(1, 0, 2, 3).reshape(LEN * IMAGES, HW)
    projected = jnp.dot(attended, out_weight, preferred_element_type=jnp.float32).reshape(LEN, IMAGES, D)
    updated = (residual_in.astype(jnp.float32) + conditions[None, :, 0, :] * projected).astype(jnp.bfloat16)
    updated_f = updated.astype(jnp.float32)
    mean_value = lax.optimization_barrier(jnp.mean(updated_f, axis=-1, keepdims=True))
    centered = updated_f - mean_value
    variance = lax.optimization_barrier(jnp.mean(centered * centered, axis=-1, keepdims=True))
    normed = centered * lax.rsqrt(variance + 1e-06)
    moe_in = (normed * (1.0 + conditions[None, :, 2, :]) + conditions[None, :, 1, :]).astype(jnp.bfloat16)
    logits = jnp.dot(moe_in.reshape(LEN * IMAGES, D), router_weight, preferred_element_type=jnp.float32)
    token_ids = jnp.swapaxes(expert_ids, 1, 2).reshape(LEN * IMAGES, TOP)
    chosen = jnp.take_along_axis(logits, token_ids, axis=1)
    first_share = jax.nn.sigmoid(chosen[:, 0] - chosen[:, 1]).reshape(LEN, IMAGES)
    block_count = N_SEQ * N_EXP
    blocks = expert_ids.reshape(block_count, -1)
    onehot = (blocks[:, :, None] == jnp.arange(EXPERTS, dtype=jnp.int32)[None, None, :]).astype(jnp.int32)
    slot_index = lax.optimization_barrier(jnp.sum(jnp.cumsum(onehot, axis=1) * onehot, axis=2)) - 1
    block_ids = jnp.arange(block_count, dtype=jnp.int32)[:, None]
    flat_index = (blocks * (block_count * CAP) + block_ids * CAP + slot_index).astype(jnp.int32).reshape(-1)
    block_rows = jnp.repeat(to_blocks(moe_in), TOP, axis=1).reshape(-1, D)
    buffer = jnp.zeros((EXPERTS * block_count * CAP, D), jnp.bfloat16).at[flat_index].set(block_rows)
    first_pairs = first_weight.reshape(EXPERTS, 2, D, FFW // 2)
    second_pairs = second_weight.reshape(EXPERTS, 2, FFW // 2, D)
    out_buffer = lax.map(expert_apply, (buffer.reshape(EXPERTS, block_count * CAP, D), first_pairs, second_pairs))
    returned = out_buffer.reshape(-1, D)[flat_index].reshape(block_count, -1, TOP, D).astype(jnp.float32)
    share_blocks = to_blocks(first_share[:, :, None])[:, :, 0]
    mixed_out = share_blocks[:, :, None] * returned[:, :, 0, :] + (1.0 - share_blocks)[:, :, None] * returned[:, :, 1, :]
    moe_out = from_blocks(mixed_out)
    return (updated_f + conditions[None, :, 3, :] * moe_out).astype(jnp.bfloat16)
```

```python
import functools
import math

import jax
import jax.numpy as jnp
from jax import lax
from jax.experimental import pallas as pl
from jax.experimental.pallas import tpu as pltpu
from jax.sharding import PartitionSpec as P

HEAD = 72
FREQ = 256
BF16 = jnp.bfloat16
F32 = jnp.float32


def swapped(block, axis, offset):
    if offset == 0:
        return block
    count = lax.axis_size(axis)
    return lax.ppermute(block, axis, [(place, place ^ offset) for place in range(count)])


def vmem():
    return pl.BlockSpec(memory_space=pltpu.VMEM)


def smem():
    return pl.BlockSpec(memory_space=pltpu.SMEM)


def call(kernel, name, scalars, arrays, outs, scratch=(), flops=0):
    return pl.pallas_call(
        kernel,
        name=name,
        in_specs=[smem() for _ in scalars] + [vmem() for _ in arrays],
        out_specs=[vmem() for _ in outs],
        out_shape=[jax.ShapeDtypeStruct(shape, dtype) for shape, dtype in outs],
        scratch_shapes=list(scratch),
        cost_estimate=pl.CostEstimate(flops=flops, transcendentals=0, bytes_accessed=0),
    )(*scalars, *arrays)


def time_embed(timesteps):
    half_width = FREQ // 2
    frequencies = jnp.exp(
        -math.log(10000.0) * jnp.arange(half_width, dtype=jnp.float32) / half_width
    )
    angles = timesteps.astype(jnp.float32)[:, None] * frequencies[None, :]
    return jnp.concatenate([jnp.cos(angles), jnp.sin(angles)], axis=1)


def modulation(class_table, time_weight, class_labels, timesteps, seq_place, seq_count):
    table_rows = class_table.shape[0]
    own_row = class_labels[0] - seq_place * table_rows
    held = (own_row >= 0) & (own_row < table_rows)
    picked = lax.dynamic_slice_in_dim(
        class_table, jnp.clip(own_row, 0, table_rows - 1), 1, 0
    )[0].astype(F32)
    class_part = jnp.where(held, picked, 0.0)
    freq_rows = time_weight.shape[0]
    own_freq = lax.dynamic_slice_in_dim(
        time_embed(timesteps)[0], seq_place * freq_rows, freq_rows, 0
    )
    time_part = jnp.sum(own_freq[:, None, None] * time_weight.astype(F32), axis=0)
    total = class_part + time_part
    offset = 1
    while offset < seq_count:
        total = total + swapped(total, "seq", offset)
        offset *= 2
    return total


def pack_kernel(place_ref, q_ref, k_ref, v_ref, *rest):
    count = len(rest) - 1
    outs, held = rest[:count], rest[count]
    width = q_ref.shape[1] // count
    place = place_ref[0]
    for member in range(count):
        cut = slice(member * width, (member + 1) * width)
        held[member ^ place] = jnp.concatenate(
            [q_ref[:, cut], k_ref[:, cut], v_ref[:, cut]], axis=1
        )
    for offset in range(count):
        outs[offset][...] = held[offset]


def attention_kernel(*refs, count, fold):
    ins, outs = refs[:count], refs[count : 2 * count]
    key_held, value_held = refs[2 * count :]
    width = ins[0].shape[1] // 3
    rows = ins[0].shape[0]
    heads = width // HEAD
    scale = math.log2(math.e) / math.sqrt(HEAD)
    for head in range(heads):
        for offset in range(count):
            block = slice(offset * rows, (offset + 1) * rows)
            low = width + head * HEAD
            key_held[head, block, :] = ins[offset][:, low : low + HEAD]
            low = 2 * width + head * HEAD
            value_held[head, block, :] = jnp.concatenate(
                [ins[offset][:, low : low + HEAD], jnp.ones((rows, 128 - HEAD), BF16)], axis=1
            )
    for offset in range(count):
        pieces = []
        for head in range(heads):
            query = ins[offset][:, head * HEAD : (head + 1) * HEAD]
            scores = lax.dot_general(
                query, key_held[head], (((1,), (1,)), ((), ())), preferred_element_type=F32
            )
            row_max = jnp.max(scores, axis=1, keepdims=True)
            weights = jnp.exp2((scores - row_max) * scale).astype(BF16)
            mixed = jnp.dot(weights, value_held[head], preferred_element_type=F32)
            pieces.append((mixed[:, :HEAD] / mixed[:, HEAD : HEAD + 1]).astype(BF16))
        joined = jnp.concatenate(pieces, axis=1)
        step = rows // fold
        outs[offset][...] = jnp.concatenate(
            [joined[part * step : (part + 1) * step, :] for part in range(fold)], axis=1
        )


def project_kernel(place_ref, residual_ref, cond_ref, weight_ref, *rest, count, fold):
    blocks, updated_ref, outs = rest[:count], rest[count], rest[count + 1 :]
    width = weight_ref.shape[0] // count
    place = place_ref[0]
    unfolded, weights = [], []
    for offset in range(count):
        block = blocks[offset][...]
        unfolded.append(
            jnp.concatenate(
                [block[:, part * width : (part + 1) * width] for part in range(fold)], axis=0
            )
        )
        low = pl.multiple_of((place ^ offset) * width, 8)
        weights.append(weight_ref[pl.ds(low, width), :])
    projected = jnp.dot(
        jnp.concatenate(unfolded, axis=1),
        jnp.concatenate(weights, axis=0),
        preferred_element_type=F32,
    )
    updated = (residual_ref[...].astype(F32) + cond_ref[0:1, :] * projected).astype(BF16)
    updated_ref[...] = updated
    updated_f = updated.astype(F32)
    centered = updated_f - jnp.mean(updated_f, axis=1, keepdims=True)
    variance = jnp.mean(centered * centered, axis=1, keepdims=True)
    normed = centered * lax.rsqrt(variance + 1e-06)
    moe_in = (normed * (1.0 + cond_ref[2:3, :]) + cond_ref[1:2, :]).astype(BF16)
    chunk = outs[0].shape[1]
    for index, out in enumerate(outs):
        out[...] = moe_in[:, index * chunk : (index + 1) * chunk]


def dispatch_kernel(place_ref, ids_ref, *rest, parts):
    ins, outs = rest[:parts], rest[parts:]
    place = place_ref[0]
    tokens = ids_ref.shape[1]
    slots = outs[0].shape[0]
    count = len(outs)
    lane_expert = place ^ lax.broadcasted_iota(jnp.int32, (count, tokens), 0)
    named = (ids_ref[0:1, :] == lane_expert) | (ids_ref[1:2, :] == lane_expert)
    before = lax.broadcasted_iota(jnp.int32, (tokens, tokens), 0) < lax.broadcasted_iota(
        jnp.int32, (tokens, tokens), 1
    )
    ordinal = jnp.dot(
        named.astype(F32).astype(BF16),
        before.astype(F32).astype(BF16),
        preferred_element_type=F32,
    )
    ordinal = jnp.where(named, ordinal, -1.0)
    slot = lax.broadcasted_iota(jnp.int32, (slots, tokens), 0).astype(F32)
    for offset in range(count):
        choice = (ordinal[offset : offset + 1, :] == slot).astype(F32).astype(BF16)
        outs[offset][...] = jnp.concatenate(
            [jnp.dot(choice, piece[...], preferred_element_type=F32) for piece in ins], axis=1
        ).astype(BF16)


def route_kernel(place_ref, ids_ref, router_ref, *rest, parts):
    ins, share_ref, slot_ref = rest[:parts], rest[parts], rest[parts + 1]
    place = place_ref[0]
    tokens = ids_ref.shape[0]
    experts = router_ref.shape[1]
    first, second = ids_ref[:, 0:1], ids_ref[:, 1:2]
    chunk = ins[0].shape[1]
    logits = jnp.zeros((tokens, experts), F32)
    for index in range(parts):
        logits = logits + jnp.dot(
            ins[index][...],
            router_ref[index * chunk : (index + 1) * chunk, :],
            preferred_element_type=F32,
        )
    lane = lax.broadcasted_iota(jnp.int32, (tokens, experts), 1)
    first_logit = jnp.sum(jnp.where(lane == first, logits, 0.0), axis=1, keepdims=True)
    second_logit = jnp.sum(jnp.where(lane == second, logits, 0.0), axis=1, keepdims=True)
    share = 1.0 / (1.0 + jnp.exp(second_logit - first_logit))
    lane_expert = place ^ lax.broadcasted_iota(jnp.int32, share_ref.shape, 1)
    is_first, is_second = lane_expert == first, lane_expert == second
    share_ref[...] = jnp.where(is_first, share, 0.0) + jnp.where(is_second, 1.0 - share, 0.0)
    named = is_first | is_second
    before = lax.broadcasted_iota(jnp.int32, (tokens, tokens), 1) < lax.broadcasted_iota(
        jnp.int32, (tokens, tokens), 0
    )
    ordinal = jnp.dot(
        before.astype(F32).astype(BF16),
        named.astype(F32).astype(BF16),
        preferred_element_type=F32,
    )
    slot_ref[...] = jnp.where(named, ordinal, -1.0)


def combine_kernel(share_ref, slot_ref, *rest):
    blocks, out_ref = rest[:-1], rest[-1]
    slots = blocks[0].shape[0]
    tokens = share_ref.shape[0]
    lane = lax.broadcasted_iota(jnp.int32, (tokens, slots), 1).astype(F32)
    total = None
    for offset, block in enumerate(blocks):
        choice = (slot_ref[:, offset : offset + 1] == lane).astype(F32).astype(BF16)
        picked = jnp.dot(choice, block[...], preferred_element_type=F32)
        picked = share_ref[:, offset : offset + 1] * picked
        total = picked if total is None else total + picked
    out_ref[...] = total.astype(out_ref.dtype)


def hidden_kernel(weight_ref, *rest, parts):
    out_ref, joined = rest[-2], rest[-1]
    blocks = rest[:-2]
    slots, chunk = blocks[0].shape

    @pl.when(pl.program_id(0) == 0)
    def _():
        for index, block in enumerate(blocks):
            row, column = index // parts, index % parts
            joined[row * slots : (row + 1) * slots, column * chunk : (column + 1) * chunk] = block[
                ...
            ]

    pre_act = jnp.dot(joined[...], weight_ref[...], preferred_element_type=F32)
    out_ref[...] = jax.nn.gelu(pre_act, approximate=True).astype(BF16)


def expert_out_kernel(hidden_ref, *rest, pieces):
    weights, outs = rest[:pieces], rest[pieces:]
    weight = jnp.concatenate([piece[...] for piece in weights], axis=0)
    total = jnp.dot(hidden_ref[...], weight, preferred_element_type=F32).astype(BF16)
    slots = outs[0].shape[0]
    for index, out in enumerate(outs):
        out[...] = total[index * slots : (index + 1) * slots, :]


def finish_kernel(updated_ref, cond_ref, own_ref, *rest):
    mirrored, out_ref = rest[:-1], rest[-1]
    chunk = mirrored[0].shape[1]
    for index, piece in enumerate(mirrored):
        cut = slice(index * chunk, (index + 1) * chunk)
        moe_out = own_ref[:, cut] + piece[...].astype(F32)
        out_ref[:, cut] = (
            updated_ref[:, cut].astype(F32) + cond_ref[3:4, cut] * moe_out
        ).astype(BF16)


def hidden_units(blocks, weight, parts):
    depth, units = weight.shape
    slots = blocks[0].shape[0]
    rows = slots * len(blocks) // parts
    block = next(size for size in (768, 512, 384, 256, 128) if units % size == 0)
    return pl.pallas_call(
        functools.partial(hidden_kernel, parts=parts),
        name="hidden_units",
        grid=(units // block,),
        in_specs=[pl.BlockSpec((depth, block), lambda i: (0, i))]
        + [pl.BlockSpec(piece.shape, lambda i: (0, 0)) for piece in blocks],
        out_specs=pl.BlockSpec((rows, block), lambda i: (0, i)),
        out_shape=jax.ShapeDtypeStruct((rows, units), BF16),
        scratch_shapes=[pltpu.VMEM((rows, depth), BF16)],
        cost_estimate=pl.CostEstimate(
            flops=2 * rows * depth * units, transcendentals=0, bytes_accessed=0
        ),
    )(weight, *blocks)


def expert_out(hidden, weights, index, chunk, count):
    rows, units = hidden.shape
    slots = rows // count
    return pl.pallas_call(
        functools.partial(expert_out_kernel, pieces=len(weights)),
        name="expert_out",
        grid=(1,),
        in_specs=[pl.BlockSpec(hidden.shape, lambda i: (0, 0))]
        + [pl.BlockSpec((piece.shape[0], chunk), lambda i: (0, index)) for piece in weights],
        out_specs=[pl.BlockSpec((slots, chunk), lambda i: (0, 0)) for _ in range(count)],
        out_shape=[jax.ShapeDtypeStruct((slots, chunk), BF16) for _ in range(count)],
        cost_estimate=pl.CostEstimate(
            flops=2 * rows * units * chunk, transcendentals=0, bytes_accessed=0
        ),
    )(hidden, *weights)


def body(
    residual_in,
    query_proj,
    key_proj,
    value_proj,
    out_weight,
    router_weight,
    first_weight,
    second_weight,
    class_table,
    time_weight,
    class_labels,
    timesteps,
    expert_ids,
):
    tokens, images, model_width = residual_in.shape
    assert images == 1
    seq_count, exp_count = lax.axis_size("seq"), lax.axis_size("exp")
    experts = router_weight.shape[1]
    siblings = exp_count // experts
    seq_place = lax.axis_index("seq")
    column = lax.axis_index("exp") // siblings
    seq_scalar = seq_place.astype(jnp.int32).reshape(1)
    column_scalar = column.astype(jnp.int32).reshape(1)
    residual, query, key, value = (
        array.reshape(tokens, model_width)
        for array in (residual_in, query_proj, key_proj, value_proj)
    )
    mirror = seq_count // 2
    top_count = expert_ids.shape[-1]
    capacity = max(2, 5 * tokens * top_count // (4 * experts))
    slots = -(-capacity // 16) * 16
    chunk = 384 if model_width % 384 == 0 else model_width
    parts = model_width // chunk
    fold = seq_count if tokens % (16 * seq_count) == 0 else 1
    head_width = query.shape[1] // seq_count

    conditions = modulation(
        class_table, time_weight, class_labels, timesteps, seq_place, seq_count
    )
    packed = call(
        pack_kernel,
        "pack",
        [seq_scalar],
        [query, key, value],
        [((tokens, 3 * head_width), BF16)] * seq_count,
        [pltpu.VMEM((seq_count, tokens, 3 * head_width), BF16)],
    )
    packed = [swapped(block, "seq", offset) for offset, block in enumerate(packed)]

    ids = expert_ids.reshape(tokens, top_count)
    ids_mirror = swapped(ids, "seq", mirror)

    first_own, second_own = first_weight[0], second_weight[0]
    first_pieces, second_pieces = [], []
    for offset in range(mirror):
        first_piece = swapped(first_own, "seq", offset)
        second_piece = swapped(second_own, "seq", offset)
        for sibling in range(siblings):
            first_pieces.append(swapped(first_piece, "exp", sibling))
            second_pieces.append(swapped(second_piece, "exp", sibling))
    first_all = jnp.concatenate(first_pieces, axis=1)

    mixed = call(
        functools.partial(attention_kernel, count=seq_count, fold=fold),
        "attention",
        [],
        packed,
        [((tokens // fold, fold * head_width), BF16)] * seq_count,
        [
            pltpu.VMEM((head_width // HEAD, seq_count * tokens, HEAD), BF16),
            pltpu.VMEM((head_width // HEAD, seq_count * tokens, 128), BF16),
        ],
        flops=4 * tokens * tokens * seq_count * seq_count * head_width,
    )
    mixed = [swapped(block, "seq", offset) for offset, block in enumerate(mixed)]
    updated, *moe_own = call(
        functools.partial(project_kernel, count=seq_count, fold=fold),
        "project",
        [seq_scalar],
        [residual, conditions, out_weight, *mixed],
        [((tokens, model_width), BF16)] + [((tokens, chunk), BF16)] * parts,
        flops=2 * tokens * model_width * model_width,
    )
    moe_mirror = [swapped(piece, "seq", mirror) for piece in moe_own]

    def dispatch(pieces, id_rows):
        return call(
            functools.partial(dispatch_kernel, parts=len(pieces)),
            "dispatch",
            [column_scalar],
            [id_rows, *pieces],
            [((slots, chunk * len(pieces)), BF16)] * experts,
            flops=2 * tokens * slots * experts * chunk * len(pieces),
        )

    def route(pieces, id_columns):
        return call(
            functools.partial(route_kernel, parts=parts),
            "route",
            [column_scalar],
            [id_columns, router_weight, *pieces],
            [((tokens, 128), F32), ((tokens, 128), F32)],
            flops=2 * tokens * tokens * 128,
        )

    def exchange(blocks):
        return [swapped(block, "exp", siblings * offset) for offset, block in enumerate(blocks)]

    def combine(shares, blocks, dtype):
        return call(
            combine_kernel,
            "combine",
            [],
            [*shares, *blocks],
            [((tokens, blocks[0].shape[1]), dtype)],
            flops=2 * tokens * slots * experts * blocks[0].shape[1],
        )[0]

    arrived_own = exchange(dispatch(moe_own, ids.T))
    shares_own = route(moe_own, ids)
    arrived = [exchange(dispatch([piece], ids_mirror.T)) for piece in moe_mirror]
    shares_mirror = route(moe_mirror, ids_mirror)

    hidden_own = hidden_units(arrived_own, first_all, 1)
    hidden_mirror = hidden_units(
        [arrived[part][offset] for offset in range(experts) for part in range(parts)],
        first_all,
        parts,
    )
    sent_back = []
    for part in range(parts):
        blocks = exchange(expert_out(hidden_mirror, second_pieces, part, chunk, experts))
        sent_back.append(swapped(combine(shares_mirror, blocks, BF16), "seq", mirror))
    own_blocks = exchange(expert_out(hidden_own, second_pieces, 0, model_width, experts))
    own_total = combine(shares_own, own_blocks, F32)
    block_out = call(
        finish_kernel,
        "finish",
        [],
        [updated, conditions, own_total, *sent_back],
        [((tokens, model_width), BF16)],
    )[0]
    return block_out.reshape(tokens, 1, model_width)


def solution(mesh):
    return jax.shard_map(
        body,
        mesh=mesh,
        in_specs=(
            P("seq", "exp", None),
            P("seq", "exp", None),
            P("seq", "exp", None),
            P("seq", "exp", None),
            P(),
            P(),
            P("exp", None, "seq"),
            P("exp", "seq", None),
            P("seq", None, None),
            P("seq", None, None),
            P("exp"),
            P("exp"),
            P("seq", "exp", None, None, None),
        ),
        out_specs=P("seq", "exp", None),
        check_vma=False,
    )
```
